32 devices in a mesh: grp: 8 (over y, x, core), tp: 4 (over z).
Axes of the slice: x: 2, y: 2, z: 4, core: 2. Of those that a mesh axis runs over, the one named last changes fastest.
Arguments:
- tokens: bfloat16 [4096, 6144], P('grp'), may hold values from -40 to 40
- norm_gain: bfloat16 [6144], replicated, may hold values from 0.099609375 to 1.8984375
- up_weight: bfloat16 [6144, 12288], P('grp', 'tp'), may hold values from -0.078125 to 0.078125
- up_bias: float32 [12288], P('tp'), may hold values from -3 to 3
- down_weight: bfloat16 [12288, 6144], P('tp', 'grp'), may hold values from -0.0546875 to 0.0546875
- down_bias: float32 [6144], P('tp'), may hold values from -2 to 2
Outputs:
- encoded: bfloat16 [4096, 6144], P('grp', 'tp')
The draws below stay inside these ranges and needn't reach their ends.
All inputs are finite; a program needn't handle non-finite values.
Results may differ from the reference program's by a relative error of at most 0.0085.
Values may be sent and summed in bfloat16 or wider, within the bound.
A program may use at most 128 MiB of HBM per device.

```python
import jax
import jax.numpy as jnp
from jax import lax

D = 6144
FF = 12288
ROWS = 4096
N_TP = 4


def draw_tokens(key, part):
    keys = jax.random.split(key, 4)
    offsets = jax.random.uniform(keys[0], (16,), jnp.float32, -0.5, 0.5)
    column = jax.random.uniform(keys[1], (D,), jnp.float32, -0.5, 0.5) + jnp.repeat(offsets, D // 16)
    column_scale = 10.0 ** column
    row_scale = jnp.exp(jax.random.uniform(keys[2], (ROWS, 1), jnp.float32, -0.69, 0.69))
    base = jnp.clip(jax.random.normal(keys[3], (ROWS, D), jnp.float32), -6.0, 6.0)
    return jnp.clip(base * column_scale * row_scale, -40.0, 40.0).astype(jnp.bfloat16)


def block_scale(own_key, extent, pieces, low, largest):
    loudness, own = 1.0, jax.random.fold_in(own_key, 6)
    for dim, shards_of in pieces:
        steps = jnp.exp(jax.random.uniform(jax.random.fold_in(own, dim), (shards_of,), jnp.float32, low / len(pieces), largest / len(pieces)))
        loudness = loudness * jnp.repeat(steps, extent[dim] // shards_of).reshape([-1 if axis == dim else 1 for axis in range(len(extent))])
    return loudness


def bell_draw(rng, shape, spread, bound, shards=(), held_as=jnp.bfloat16):
    array = spread * jax.random.normal(rng, shape, jnp.float32)
    if shards:
        array = array * block_scale(rng, shape, shards, -0.22, 0.18)
    return jnp.clip(array, -bound, bound).astype(held_as)


def setup_inputs(seed: int = 0) -> dict:
    key_list = jax.random.split(jax.random.key(seed), 7)
    return {
        "tokens": draw_tokens(jax.random.fold_in(key_list[6], 71), 0),
        "norm_gain": jnp.clip(1.0 + 0.18 * jax.random.normal(key_list[1], (D,), jnp.float32), 0.099609375, 1.8984375).astype(jnp.bfloat16),
        "up_weight": bell_draw(key_list[2], (D, FF), D ** -0.5, 0.078125, ((0, 8), (1, 4))),
        "up_bias": bell_draw(key_list[3], (FF,), 0.5, 3.0, ((0, 4),), jnp.float32),
        "down_weight": bell_draw(key_list[4], (FF, D), FF ** -0.5, 0.0546875, ((0, 4), (1, 8))),
        "down_bias": bell_draw(key_list[5], (D,), 0.3, 2.0, ((0, 4),), jnp.float32),
    }


def reference(tokens, norm_gain, up_weight, up_bias, down_weight, down_bias):
    values = tokens.astype(jnp.float32)
    centre = lax.optimization_barrier(jnp.mean(values, axis=1, keepdims=True))
    shifted = values - centre
    variance = lax.optimization_barrier(jnp.mean(shifted * shifted, axis=1, keepdims=True))
    normed = (shifted * lax.rsqrt(variance + 1e-06) * norm_gain.astype(jnp.float32)).astype(jnp.bfloat16)
    pre = jnp.dot(normed, up_weight, preferred_element_type=jnp.float32) + up_bias
    hidden = jax.nn.gelu(pre, approximate=True).astype(jnp.bfloat16)
    width = FF // N_TP
    summed = jnp.zeros(values.shape, jnp.float32)
    for index in range(N_TP):
        term = jnp.dot(hidden[:, index * width:(index + 1) * width], down_weight[index * width:(index + 1) * width, :], preferred_element_type=jnp.float32)
        rounded = lax.optimization_barrier(term.astype(jnp.bfloat16))
        summed = summed + rounded.astype(jnp.float32)
    return (values + summed + down_bias).astype(jnp.bfloat16)
```

```python
import jax
import jax.numpy as jnp
from jax import lax
from jax.sharding import PartitionSpec as P

UP_CHUNKS = 4
DOWN_CHUNKS = 3


def after(value, *deps):
    return lax.optimization_barrier((value,) + deps)[0]


def split_of(extent, wanted):
    count = wanted
    while count > 1 and extent % (count * 128):
        count -= 1
    return count


def build(groups, planes):
    bits = groups.bit_length() - 1
    up_bit, down_bit = bits - 1, min(1, bits - 1)
    every = list(range(bits))[1:] + [0]

    def flip(value, bit):
        return lax.ppermute(value, "grp", [(i, i ^ (1 << bit)) for i in range(groups)])

    def masks_of(skip):
        masks = [0]
        for bit in every:
            if bit != skip:
                masks = masks + [m ^ (1 << bit) for m in masks]
        return masks

    def collect(block, skip):
        parts = [block]
        first = None
        for bit in every:
            if bit != skip:
                parts = parts + [flip(part, bit) for part in parts]
                first = parts[-1] if first is None else first
        return parts, first

    def per_device(tokens, norm_gain, up_weight, up_bias, down_weight, down_bias):
        me = lax.axis_index("grp")
        plane = lax.axis_index("tp")
        depth, hidden_width = up_weight.shape
        out_block = down_weight.shape[1]
        half = tokens.shape[1] // 2
        half_blocks = groups // 2
        up_masks, down_masks = masks_of(up_bit), masks_of(down_bit)

        my_half = me // half_blocks
        partner_raw = flip(
            lax.dynamic_slice_in_dim(tokens, (1 - my_half) * half, half, 1), up_bit
        )

        up_count = split_of(hidden_width, UP_CHUNKS)
        up_step = hidden_width // up_count
        up_parts, firsts = [], []
        for j in range(up_count):
            piece = up_weight[:, j * up_step:(j + 1) * up_step]
            if j >= 2:
                piece = after(piece, firsts[j - 2])
            parts, first = collect(piece, up_bit)
            up_parts.append(parts)
            firsts.append(first)

        values = tokens.astype(jnp.float32)
        centre = jnp.mean(values, axis=1, keepdims=True)
        shifted = values - centre
        variance = jnp.mean(shifted * shifted, axis=1, keepdims=True)
        scale = lax.rsqrt(variance + 1e-06)
        stats = jnp.concatenate([centre.T, scale.T], axis=0)
        partner_stats = flip(stats, up_bit)

        def block_of(array, index, axis):
            return lax.dynamic_slice_in_dim(array, index * depth, depth, axis)

        gain = jnp.concatenate([block_of(norm_gain, me ^ m, 0) for m in up_masks]).astype(jnp.float32)

        def normalise(raw, mean, inverse):
            return ((raw.astype(jnp.float32) - mean) * inverse * gain).astype(jnp.bfloat16)

        own_normed = normalise(
            jnp.concatenate([block_of(tokens, me ^ m, 1) for m in up_masks], axis=1), centre, scale
        )
        inner = me % half_blocks
        partner_normed = normalise(
            jnp.concatenate([block_of(partner_raw, inner ^ m, 1) for m in up_masks], axis=1),
            partner_stats[0][:, None],
            partner_stats[1][:, None],
        )

        own_hidden, other_hidden = [], []
        last_sent = None
        for j in range(up_count):
            weight = jnp.concatenate(up_parts[j], axis=0)
            sent = jnp.dot(
                partner_normed, weight, preferred_element_type=jnp.float32
            ).astype(jnp.bfloat16)
            received = flip(sent, up_bit)
            last_sent = sent
            own = jnp.dot(own_normed, weight, preferred_element_type=jnp.float32)
            pre = own + received.astype(jnp.float32) + up_bias[j * up_step:(j + 1) * up_step]
            piece = jax.nn.gelu(pre, approximate=True).astype(jnp.bfloat16)
            own_hidden.append(piece)
            other_hidden.append(flip(piece, down_bit))
        own_hidden = jnp.concatenate(own_hidden, axis=1)
        other_hidden = jnp.concatenate(other_hidden, axis=1)

        down_count = split_of(out_block, DOWN_CHUNKS)
        down_step = out_block // down_count
        per_plane = groups // planes
        firsts = [last_sent, last_sent]
        down_parts = []
        for q in range(down_count):
            piece = after(down_weight[:, q * down_step:(q + 1) * down_step], firsts[q])
            parts, first = collect(piece, down_bit)
            down_parts.append(parts)
            firsts.append(first)

        own_width = down_bias.shape[0]
        own_tokens = lax.dynamic_slice_in_dim(tokens, plane * own_width, own_width, 1)
        pieces = []
        for q in range(down_count):
            weight = jnp.concatenate(down_parts[q], axis=1)
            theirs = jnp.dot(
                other_hidden, weight, preferred_element_type=jnp.float32
            ).astype(jnp.bfloat16)
            received = flip(theirs, down_bit)
            mine = jnp.dot(
                own_hidden, weight, preferred_element_type=jnp.float32
            ).astype(jnp.bfloat16)
            located = {}
            for position, m in enumerate(down_masks):
                columns = slice(position * down_step, (position + 1) * down_step)
                located[m] = mine[:, columns]
                located[m ^ (1 << down_bit)] = received[:, columns]
            stacked = jnp.stack([located[m] for m in range(groups)])

            def for_plane(target):
                return jnp.concatenate(
                    [
                        lax.dynamic_index_in_dim(
                            stacked, (target * per_plane + i) ^ me, 0, keepdims=False
                        )
                        for i in range(per_plane)
                    ],
                    axis=1,
                )

            total = for_plane(plane).astype(jnp.float32)
            for d in range(1, planes):
                moved = lax.ppermute(
                    for_plane((plane + d) % planes),
                    "tp",
                    [(t, (t + d) % planes) for t in range(planes)],
                )
                total = total + moved.astype(jnp.float32)
            pieces.append(total)
        summed = jnp.concatenate(
            [
                pieces[q][:, i * down_step:(i + 1) * down_step]
                for i in range(per_plane)
                for q in range(down_count)
            ],
            axis=1,
        )
        return (own_tokens.astype(jnp.float32) + summed + down_bias).astype(jnp.bfloat16)

    return per_device


def solution(mesh):
    in_specs = (P("grp", None), P(), P("grp", "tp"), P("tp"), P("tp", "grp"), P("tp"))
    out_specs = P("grp", "tp")
    return jax.shard_map(
        build(mesh.shape["grp"], mesh.shape["tp"]),
        mesh=mesh, in_specs=in_specs, out_specs=out_specs, check_vma=False,
    )
```

```python
import jax
import jax.numpy as jnp
from jax import lax
from jax.sharding import PartitionSpec as P

UP_CHUNKS = 4
DOWN_CHUNKS = 3


def after(value, *deps):
    return lax.optimization_barrier((value,) + deps)[0]


def split_of(extent, wanted):
    count = wanted
    while count > 1 and extent % (count * 128):
        count -= 1
    return count


def build(groups, planes):
    bits = groups.bit_length() - 1
    up_bit, down_bit = bits - 1, min(1, bits - 1)
    every = list(range(bits))[1:] + [0]

    def flip(value, bit):
        return lax.ppermute(value, "grp", [(i, i ^ (1 << bit)) for i in range(groups)])

    def masks_of(skip):
        masks = [0]
        for bit in every:
            if bit != skip:
                masks = masks + [m ^ (1 << bit) for m in masks]
        return masks

    def per_device(tokens, norm_gain, up_weight, up_bias, down_weight, down_bias):
        me = lax.axis_index("grp")
        plane = lax.axis_index("tp")
        depth, hidden_width = up_weight.shape
        out_block = down_weight.shape[1]
        half = tokens.shape[1] // 2
        half_blocks = groups // 2
        up_masks, down_masks = masks_of(up_bit), masks_of(down_bit)

        my_half = me // half_blocks
        partner_raw = flip(
            lax.dynamic_slice_in_dim(tokens, (1 - my_half) * half, half, 1), up_bit
        )

        up_count = split_of(hidden_width, UP_CHUNKS)
        up_step = hidden_width // up_count
        up_parts, firsts = [], []
        for j in range(up_count):
            piece = up_weight[:, j * up_step:(j + 1) * up_step]
            if j >= 2:
                piece = after(piece, firsts[j - 2])
            parts = [piece]
            for bit in every[:-1]:
                if bit != up_bit:
                    parts = parts + [flip(part, bit) for part in parts]
            up_parts.append(parts)
            firsts.append(parts[-1])

        values = tokens.astype(jnp.float32)
        centre = jnp.mean(values, axis=1, keepdims=True)
        shifted = values - centre
        variance = jnp.mean(shifted * shifted, axis=1, keepdims=True)
        scale = lax.rsqrt(variance + 1e-06)
        stats = jnp.concatenate([centre.T, scale.T], axis=0)
        partner_stats = flip(stats, up_bit)

        def block_of(array, index, axis):
            return lax.dynamic_slice_in_dim(array, index * depth, depth, axis)

        gain = jnp.concatenate([block_of(norm_gain, me ^ m, 0) for m in up_masks]).astype(jnp.float32)

        def normalise(raw, mean, inverse):
            return ((raw.astype(jnp.float32) - mean) * inverse * gain).astype(jnp.bfloat16)

        own_normed = normalise(
            jnp.concatenate([block_of(tokens, me ^ m, 1) for m in up_masks], axis=1), centre, scale
        )
        inner = me % half_blocks
        partner_normed = normalise(
            jnp.concatenate([block_of(partner_raw, inner ^ m, 1) for m in up_masks], axis=1),
            partner_stats[0][:, None],
            partner_stats[1][:, None],
        )

        own_hidden, other_hidden = [], []
        sents, arrivals = [], []
        for j in range(up_count):
            parts = up_parts[j]
            if j >= 2:
                parts = list(lax.optimization_barrier((*parts, sents[j - 2]))[:-1])
            weight = jnp.concatenate(parts + [flip(part, every[-1]) for part in parts], axis=0)
            sent = jnp.dot(
                partner_normed, weight, preferred_element_type=jnp.float32
            ).astype(jnp.bfloat16)
            received = flip(sent, up_bit)
            sents.append(sent)
            arrivals.append(received)
            own = jnp.dot(own_normed, weight, preferred_element_type=jnp.float32)
            pre = own + received.astype(jnp.float32) + up_bias[j * up_step:(j + 1) * up_step]
            piece = jax.nn.gelu(pre, approximate=True).astype(jnp.bfloat16)
            own_hidden.append(piece)
            other_hidden.append(flip(piece, down_bit))
        own_hidden = jnp.concatenate(own_hidden, axis=1)
        other_hidden = jnp.concatenate(other_hidden, axis=1)

        down_count = split_of(out_block, DOWN_CHUNKS)
        down_step = out_block // down_count
        per_plane = groups // planes
        holds = [arrivals[max(up_count - 2, 0)], arrivals[-1]]
        own_width = down_bias.shape[0]
        own_tokens = lax.dynamic_slice_in_dim(tokens, plane * own_width, own_width, 1)
        pieces, down_parts = [], []
        for q in range(down_count):
            for ahead in ((0, 1) if q == 0 else (q + 1,)):
                if ahead < down_count:
                    piece = down_weight[:, ahead * down_step:(ahead + 1) * down_step]
                    parts = [after(piece, holds[ahead])]
                    for bit in every[:-1]:
                        if bit != down_bit:
                            parts = parts + [flip(part, bit) for part in parts]
                    down_parts.append(parts)
            parts = down_parts[q]
            if q:
                parts = list(lax.optimization_barrier((*parts, holds[q + 1]))[:-1])
            weight = jnp.concatenate(parts + [flip(part, every[-1]) for part in parts], axis=1)
            theirs = jnp.dot(
                other_hidden, weight, preferred_element_type=jnp.float32
            ).astype(jnp.bfloat16)
            holds.append(theirs)
            received = flip(after(theirs, released) if q > 1 else theirs, down_bit)
            mine = jnp.dot(
                own_hidden, weight, preferred_element_type=jnp.float32
            ).astype(jnp.bfloat16)
            located = {}
            for position, m in enumerate(down_masks):
                columns = slice(position * down_step, (position + 1) * down_step)
                located[m] = mine[:, columns]
                located[m ^ (1 << down_bit)] = received[:, columns]
            stacked = jnp.stack([located[m] for m in range(groups)])

            def blocks_for(targets):
                return jnp.concatenate(
                    [
                        lax.dynamic_index_in_dim(
                            stacked, (target * per_plane + i) ^ me, 0, keepdims=False
                        )
                        for target in targets
                        for i in range(per_plane)
                    ],
                    axis=1,
                )

            low = plane % 2
            kept = blocks_for([2 * u + low for u in range(planes // 2)]).astype(jnp.float32)
            outgoing = blocks_for([2 * u + 1 - low for u in range(planes // 2)])
            released = outgoing
            width = per_plane * down_step
            for level in range(planes.bit_length() - 1):
                if level:
                    mine_bit = (plane >> level) % 2
                    count = kept.shape[1] // width // 2

                    def chosen(bit):
                        return jnp.concatenate(
                            [
                                lax.dynamic_slice_in_dim(kept, (2 * v + bit) * width, width, 1)
                                for v in range(count)
                            ],
                            axis=1,
                        )

                    outgoing = chosen(1 - mine_bit).astype(jnp.bfloat16)
                    kept = chosen(mine_bit)
                moved = lax.ppermute(
                    outgoing, "tp", [(t, t ^ (1 << level)) for t in range(planes)]
                )
                kept = kept + moved.astype(jnp.float32)
            total = kept
            pieces.append(total)
        summed = jnp.concatenate(
            [
                pieces[q][:, i * down_step:(i + 1) * down_step]
                for i in range(per_plane)
                for q in range(down_count)
            ],
            axis=1,
        )
        return (own_tokens.astype(jnp.float32) + summed + down_bias).astype(jnp.bfloat16)

    return per_device


def solution(mesh):
    in_specs = (P("grp", None), P(), P("grp", "tp"), P("tp"), P("tp", "grp"), P("tp"))
    out_specs = P("grp", "tp")
    return jax.shard_map(
        build(mesh.shape["grp"], mesh.shape["tp"]),
        mesh=mesh, in_specs=in_specs, out_specs=out_specs, check_vma=False,
    )
```
